32 devices in a mesh: groups: 2 (over y), ep: 16 (over z, x, core).
Axes of the slice: x: 2, y: 2, z: 4, core: 2. Of those that a mesh axis runs over, the one named last changes fastest.
Arguments:
- tokens: bfloat16 [4096, 1440], P(('groups', 'ep')), parts along dimension 0, may hold values from -6 to 6
- expert_ids: int32 [4096, 4], P(('groups', 'ep')), parts along dimension 0, may hold values from 0 to 15, as said below
- combine: float32 [4096, 4], P(('groups', 'ep')), parts along dimension 0, may hold values from 0.05 to 1
- gate_weight: bfloat16 [16, 1440, 1440], P('ep'), may hold values from -0.15625 to 0.15625
- up_weight: bfloat16 [16, 1440, 1440], P('ep'), may hold values from -0.15625 to 0.15625
- down_weight: bfloat16 [16, 1440, 1440], P('ep'), may hold values from -0.15625 to 0.15625
Outputs:
- mixture: bfloat16 [4096, 1440], P(('groups', 'ep')), parts along dimension 0
The draws below stay inside these ranges and needn't reach their ends.
There are 2 independent parts, one for each index of `groups`. The reference program is written for one: setup_inputs(seed, part) draws one part's arguments, and reference() takes and returns one part's arrays. A program takes and returns all parts, laid end to end along the dimension named above; an argument that names none is the same for every part. Nothing has to cross between parts.
Inputs may be any that keep to these rules, and one draw needn't show every extreme that they name: `expert_ids`: each row names 4 different experts. In the rows of one device (aligned blocks of 128 rows) no expert is named more than 64 times, and some expert is named exactly 64 times in every block.
All inputs are finite; a program needn't handle non-finite values.
Results may differ from the reference program's by a relative error of at most 0.0058.
Values may be sent and summed in bfloat16 or wider, within the bound.
A program may use at most 64 MiB of HBM per device.

```python
import math
import jax
import jax.numpy as jnp
from jax import lax

D = 1440
FF = 1440
TOP = 4
TOK_DEV = 128
EXPERTS = 16
TOKENS = 2048
CAP = 64
N_EP = 16


def route_block(key, ranking):
    cells = EXPERTS * CAP
    expert_of_cell = jnp.arange(cells, dtype=jnp.int32) // CAP
    position_in_expert = ranking[expert_of_cell]
    routing_boost = (4 << 20) // (position_in_expert + 1)
    random_jitter = jax.random.randint(jax.random.fold_in(key, 1), (cells,), 0, 1 << 20, dtype=jnp.int32)
    router_logits = routing_boost + random_jitter
    chosen = jnp.argsort(-router_logits, stable=True)[:TOK_DEV * TOP]
    listed = jnp.sort(expert_of_cell[chosen])
    table = listed.reshape(TOP, TOK_DEV).T
    random_reorder = jax.random.permutation(jax.random.fold_in(key, 2), TOK_DEV)
    return table[random_reorder]


def draw_expert_ids(key, part):
    ranking = jax.random.permutation(jax.random.fold_in(key, 7), EXPERTS).astype(jnp.int32)

    def one_block(index):
        return route_block(jax.random.fold_in(key, 100 + index), ranking)
    blocks = jax.vmap(one_block)(jnp.arange(N_EP, dtype=jnp.int32))
    return blocks.reshape(TOKENS, TOP).astype(jnp.int32)


def steps_of(own_key, dims, split, low, top_value):
    def one(axis_at, blocks):
        draws = jax.random.uniform(jax.random.fold_in(jax.random.fold_in(own_key, 6), axis_at), (blocks,), jnp.float32, low / len(split), top_value / len(split))
        return jnp.repeat(jnp.exp(draws), dims[axis_at] // blocks).reshape((-1,) + (1,) * (len(dims) - axis_at - 1))

    level = one(*split[0])
    for cut in split[1:]:
        level = level * one(*cut)
    return level


def bell_draw(key, extent, spread, reach, cuts=(), kind=jnp.bfloat16):
    entries = spread * jax.random.normal(key, extent, jnp.float32)
    if cuts:
        entries = entries * steps_of(key, extent, cuts, -0.22, 0.18)
    return jnp.clip(entries, -reach, reach).astype(kind)


def setup_inputs(seed: int = 0, part: int = 0) -> dict:
    arg_keys = jax.random.split(jax.random.key(seed), 7)
    own_keys = jax.random.split(jax.random.fold_in(arg_keys[6], part), 7)
    tokens = bell_draw(own_keys[0], (TOKENS, D), 1.0, 6.0, ((0, 16),))
    expert_ids = draw_expert_ids(jax.random.fold_in(jax.random.fold_in(arg_keys[6], part), 71), part)
    combine = jnp.clip(jnp.exp(math.log(1.0) - 2.9957323 * jax.random.uniform(own_keys[2], (TOKENS, TOP), jnp.float32) ** steps_of(own_keys[2], (TOKENS, TOP), ((0, 16),), -0.2, 0.2)), 0.05, 1.0)
    gate_weight = bell_draw(arg_keys[3], (EXPERTS, D, FF), D ** -0.5, 0.15625, ((0, 16),))
    up_weight = bell_draw(arg_keys[4], (EXPERTS, D, FF), D ** -0.5, 0.15625, ((0, 16),))
    down_weight = bell_draw(arg_keys[5], (EXPERTS, FF, D), FF ** -0.5, 0.15625, ((0, 16),))
    return dict(tokens=tokens, expert_ids=expert_ids, combine=combine, gate_weight=gate_weight, up_weight=up_weight, down_weight=down_weight)


alpha_gate = 1.702


def run_expert_block(row_block, gate_proj, up_proj, down_proj):
    gate_part = jnp.dot(row_block, gate_proj, preferred_element_type=jnp.float32)
    up_part = jnp.dot(row_block, up_proj, preferred_element_type=jnp.float32)
    hidden = ((up_part + 1.0) * gate_part * jax.nn.sigmoid(alpha_gate * gate_part)).astype(jnp.bfloat16)
    return jnp.dot(hidden, down_proj, preferred_element_type=jnp.float32).astype(jnp.bfloat16)


def reference(tokens, expert_ids, combine, gate_weight, up_weight, down_weight):
    most_rows = N_EP * CAP

    def per_expert(carry, inputs):
        expert, gate_proj, up_proj, down_proj = inputs
        chosen = expert_ids == expert
        weight_row = jnp.sum(jnp.where(chosen, combine, jnp.zeros_like(combine)), axis=1)
        present = jnp.any(chosen, axis=1)
        indices = jnp.nonzero(present, size=most_rows, fill_value=0)[0].astype(jnp.int32)
        valid = jnp.arange(most_rows, dtype=jnp.int32) < jnp.sum(present.astype(jnp.int32))
        outputs = run_expert_block(tokens[indices], gate_proj, up_proj, down_proj)
        factor = jnp.where(valid, weight_row[indices], jnp.zeros_like(weight_row[indices]))
        rescaled_logits = outputs.astype(jnp.float32) * factor[:, None]
        return carry.at[indices].add(rescaled_logits), None

    total = jnp.zeros(tokens.shape, jnp.float32)
    total, unused = lax.scan(per_expert, total, (jnp.arange(EXPERTS, dtype=jnp.int32), gate_weight, up_weight, down_weight))
    return total.astype(jnp.bfloat16)
```

```python
import functools

import jax
import jax.numpy as jnp
from jax import lax
from jax.experimental import pallas as pl
from jax.experimental.pallas import tpu as pltpu
from jax.sharding import PartitionSpec as P

MESH = pl.DeviceIdType.MESH

alpha_gate = 1.702


def run_expert_block(row_block, gate_proj, up_proj, down_proj):
    gate_part = jnp.dot(row_block, gate_proj, preferred_element_type=jnp.float32)
    up_part = jnp.dot(row_block, up_proj, preferred_element_type=jnp.float32)
    hidden = ((up_part + 1.0) * gate_part * jax.nn.sigmoid(alpha_gate * gate_part)).astype(
        jnp.bfloat16
    )
    return jnp.dot(hidden, down_proj, preferred_element_type=jnp.float32).astype(jnp.bfloat16)


def line_kernel(
    tok_hbm, mix_ref, gate_hbm, up_hbm, down_hbm, out_ref,
    x_buf, w_in, gate_w, up_w, down_w, rows, part, other, quad, rx, ru, rd,
    load_sem, agz_s, agx_s, agp_s, w_s, pc_s, rsx_s, rsz_s,
    x_r, w_r, q_r, rx_r, ru_r, rd_r,
    *, members, capacity,
):
    length = members // 4
    here = tok_hbm.shape[0]
    me = lax.axis_index("ep")
    z, x, c = me // 4, (me // 2) % 2, me % 2
    pc = 1 - c

    def member(zz, xx, cc):
        return (zz * 2 + xx) * 2 + cc

    across = member(z, 1 - x, c)
    partner = member(z, x, pc)
    above = member(jnp.minimum(z + 1, length - 1), x, c)
    below = member(jnp.maximum(z - 1, 0), x, c)

    def send(src, dst, ssem, rsem, to):
        return pltpu.make_async_remote_copy(
            src_ref=src, dst_ref=dst, send_sem=ssem, recv_sem=rsem,
            device_id={"ep": to}, device_id_type=MESH,
        )

    loads = [
        pltpu.make_async_copy(tok_hbm, x_buf.at[z, x, c], load_sem.at[0]),
        pltpu.make_async_copy(gate_hbm, gate_w, load_sem.at[1]),
        pltpu.make_async_copy(up_hbm, up_w, load_sem.at[2]),
        pltpu.make_async_copy(down_hbm, down_w, load_sem.at[3]),
    ]
    for load in loads:
        load.start()

    barrier = pltpu.get_barrier_semaphore()
    for step in range(1, members):
        to = lax.rem(me + step, members)
        pl.semaphore_signal(barrier, inc=1, device_id={"ep": to}, device_id_type=MESH)
    pl.semaphore_wait(barrier, members - 1)

    def weights_copy(step):
        to = lax.rem(me + step, members)
        return send(mix_ref.at[to], w_in.at[me], w_s.at[step], w_r.at[me], to)

    def weights_arrival(step):
        origin = lax.rem(me + step, members)
        return send(mix_ref.at[origin], w_in.at[origin], w_s.at[step], w_r.at[origin], origin)

    def ag(zz, xx, ssem, to):
        slot = x_buf.at[zz, xx, c]
        return send(slot, slot, ssem, x_r.at[zz, xx, c], to)

    def to_above(zz):
        return ag(zz, x, agz_s.at[zz, 0], above)

    def to_below(zz):
        return ag(zz, x, agz_s.at[zz, 1], below)

    def to_across(zz):
        return ag(zz, x, agx_s.at[zz], across)

    def to_partner(zz, xx):
        return ag(zz, xx, agp_s.at[zz, xx], partner)

    def goes_up(zz):
        return jnp.logical_and(zz <= z, z < length - 1)

    def goes_down(zz):
        return jnp.logical_and(zz >= z, z > 0)

    def forward(zz):
        @pl.when(goes_up(zz))
        def _():
            to_above(zz).start()

        @pl.when(goes_down(zz))
        def _():
            to_below(zz).start()

        to_across(zz).start()
        to_partner(zz, x).start()

    def arrival(zz, xx, cc):
        slot = x_buf.at[zz, xx, cc]
        send(slot, slot, agx_s.at[zz], x_r.at[zz, xx, cc], partner).wait_recv()

    near = jnp.minimum(z, length - 1 - z)

    def nearest(k):
        along = near + jnp.where(k % 2 == 1, (k + 1) // 2, -(k // 2))
        low = jnp.where(k <= 2 * near, along, k)
        return jnp.where(z == near, low, length - 1 - low)

    loads[0].wait()
    forward(z)
    for step in range(1, members):
        weights_copy(step).start()
    w_in[me] = mix_ref[me]
    for step in range(1, members):
        weights_arrival(step).wait_recv()

    row_at = lax.broadcasted_iota(jnp.int32, (capacity, here), 0).astype(jnp.float32)
    before = (
        lax.broadcasted_iota(jnp.int32, (here, here), 0)
        < lax.broadcasted_iota(jnp.int32, (here, here), 1)
    ).astype(jnp.bfloat16)

    def picker(zz, xx, cc):
        weight = w_in[member(zz, xx, cc)]
        named = weight > 0.0
        flags = jnp.broadcast_to(named.astype(jnp.float32), (8, here)).astype(jnp.bfloat16)
        rank = jnp.dot(flags, before, preferred_element_type=jnp.float32)[0:1, :]
        pick = jnp.where(named, rank, -1.0) == row_at
        scale = jnp.sum(jnp.where(pick, weight, 0.0), axis=1, keepdims=True)
        return pick.astype(jnp.float32).astype(jnp.bfloat16), scale

    def compute(zz, xx):
        picks, scales = [], []
        for side, cc in enumerate((c, pc)):
            pick, scale = picker(zz, xx, cc)
            picks.append(pick)
            scales.append(scale)
            rows[side * capacity : (side + 1) * capacity, :] = jnp.dot(
                pick, x_buf[zz, xx, cc], preferred_element_type=jnp.float32
            ).astype(jnp.bfloat16)
        block = rows[...]
        gate = jnp.dot(block, gate_w[...], preferred_element_type=jnp.float32)
        up = jnp.dot(block, up_w[...], preferred_element_type=jnp.float32)
        hidden = ((up + 1.0) * gate * jax.nn.sigmoid(alpha_gate * gate)).astype(jnp.bfloat16)
        answer = jnp.dot(hidden, down_w[...], preferred_element_type=jnp.float32)
        for side, dst in enumerate((part, other)):
            scaled = (
                answer[side * capacity : (side + 1) * capacity, :]
                .astype(jnp.bfloat16).astype(jnp.float32) * scales[side]
            ).astype(jnp.bfloat16)
            dst[zz, xx] = lax.dot_general(
                picks[side], scaled, (((0,), (0,)), ((), ())),
                preferred_element_type=jnp.float32,
            ).astype(jnp.bfloat16)

    def answer_copy(zz, xx):
        return send(other.at[zz, xx], quad.at[zz, xx], pc_s.at[zz, xx], q_r.at[zz, xx], partner)

    def across_copy(zz):
        return send(part.at[zz, 1 - x], rx.at[zz], rsx_s.at[zz], rx_r.at[zz], across)

    def join_partner(zz, xx):
        answer_copy(zz, xx).wait_recv()
        part[zz, xx] = (
            part[zz, xx].astype(jnp.float32) + quad[zz, xx].astype(jnp.float32)
        ).astype(jnp.bfloat16)

    for load in loads[1:]:
        load.wait()

    def step_of(i, carry):
        k, o = i // 2, i % 2
        zz, xx = nearest(k), (x + o) % 2

        @pl.when(o == 1)
        def _():
            @pl.when(k + 1 < length)
            def _():
                following = nearest(k + 1)
                arrival(following, x, c)
                forward(following)

            arrival(zz, 1 - x, c)
            to_partner(zz, 1 - x).start()

        arrival(zz, xx, pc)
        compute(zz, xx)
        answer_copy(zz, xx).start()

        @pl.when(i > 0)
        def _():
            last = nearest((i - 1) // 2)
            last_x = (x + (i - 1) % 2) % 2
            join_partner(last, last_x)

            @pl.when(o == 0)
            def _():
                across_copy(last).start()

        return carry

    lax.fori_loop(0, 2 * length, step_of, 0)
    final = nearest(length - 1)
    join_partner(final, 1 - x)
    across_copy(final).start()

    def up_copy(zz):
        return send(part.at[zz, x], ru.at[zz], rsz_s.at[zz], ru_r.at[zz], above)

    def down_copy(zz):
        return send(part.at[zz, x], rd.at[zz], rsz_s.at[zz], rd_r.at[zz], below)

    def chain(i, carry):
        zz = nearest(length - 1 - i)
        across_copy(zz).wait_recv()
        total = part[zz, x].astype(jnp.float32) + rx[zz].astype(jnp.float32)
        part[zz, x] = total.astype(jnp.bfloat16)

        @pl.when(jnp.logical_and(zz >= z, z > 0))
        def _():
            up_copy(zz).wait_recv()
            part[zz, x] = (
                part[zz, x].astype(jnp.float32) + ru[zz].astype(jnp.float32)
            ).astype(jnp.bfloat16)

        @pl.when(jnp.logical_and(zz <= z, z < length - 1))
        def _():
            down_copy(zz).wait_recv()
            part[zz, x] = (
                part[zz, x].astype(jnp.float32) + rd[zz].astype(jnp.float32)
            ).astype(jnp.bfloat16)

        @pl.when(zz > z)
        def _():
            up_copy(zz).start()

        @pl.when(zz < z)
        def _():
            down_copy(zz).start()

        return carry

    lax.fori_loop(0, length, chain, 0)
    out_ref[...] = part[z, x]

    for step in range(1, members):
        weights_copy(step).wait_send()

    def drain(zz, carry):
        @pl.when(goes_up(zz))
        def _():
            to_above(zz).wait_send()

        @pl.when(goes_down(zz))
        def _():
            to_below(zz).wait_send()

        to_across(zz).wait_send()
        across_copy(zz).wait_send()

        @pl.when(zz != z)
        def _():
            up_copy(zz).wait_send()

        for xx in range(2):
            to_partner(zz, xx).wait_send()
            answer_copy(zz, xx).wait_send()
        return carry

    lax.fori_loop(0, length, drain, 0)


def gathered_plan(tokens, expert_ids, combine, gate_proj, up_proj, down_proj, capacity):
    members = lax.axis_size("ep")
    here, features = tokens.shape
    ff = gate_proj.shape[1]
    length = members // 4
    experts = jnp.arange(members, dtype=jnp.int32)[:, None, None]
    ids, shares = expert_ids.T[None], combine.T[None]
    mix = jnp.sum(jnp.where(ids == experts, shares, 0.0), axis=1, keepdims=True)
    block = (here, features)
    dma = pltpu.SemaphoreType.DMA
    vmem = lambda *shape: pltpu.VMEM(shape, jnp.bfloat16)
    anywhere = pl.BlockSpec(memory_space=pl.ANY)
    inside = pl.BlockSpec(memory_space=pltpu.VMEM)
    return pl.pallas_call(
        functools.partial(line_kernel, members=members, capacity=capacity),
        out_shape=jax.ShapeDtypeStruct(block, jnp.bfloat16),
        in_specs=[anywhere, inside, anywhere, anywhere, anywhere],
        out_specs=inside,
        scratch_shapes=[
            vmem(length, 2, 2, *block),
            pltpu.VMEM((members, 1, here), jnp.float32),
            vmem(features, ff), vmem(features, ff), vmem(ff, features),
            vmem(2 * capacity, features),
            vmem(length, 2, *block), vmem(length, 2, *block), vmem(length, 2, *block),
            vmem(length, *block), vmem(length, *block), vmem(length, *block),
            dma((4,)), dma((length, 2)), dma((length,)), dma((length, 2)), dma((members,)),
            dma((length, 2)), dma((length,)), dma((length,)),
            dma((length, 2, 2)), dma((members,)), dma((length, 2)),
            dma((length,)), dma((length,)), dma((length,)),
        ],
        compiler_params=pltpu.CompilerParams(
            collective_id=0, has_side_effects=True, vmem_limit_bytes=60 * 1024 * 1024
        ),
    )(tokens, mix, gate_proj, up_proj, down_proj)


def on_device(tokens, expert_ids, combine, gate_weight, up_weight, down_weight):
    members = lax.axis_size("ep")
    tokens_here, fanout = expert_ids.shape
    features = tokens.shape[1]
    capacity = 2 * tokens_here * fanout // members
    received_rows = members * capacity
    if members % 4 == 0 and 2 * capacity >= tokens_here:
        return gathered_plan(
            tokens, expert_ids, combine, gate_weight[0], up_weight[0], down_weight[0], capacity
        )
    flat_ids = expert_ids.reshape(-1)
    onehot = (flat_ids[:, None] == jnp.arange(members, dtype=jnp.int32)[None, :]).astype(jnp.int32)
    running = jnp.cumsum(onehot, axis=0) - onehot
    slot_rank = jnp.sum(running * onehot, axis=1)
    target = flat_ids * capacity + slot_rank
    source_token = jnp.arange(tokens_here * fanout, dtype=jnp.int32) // fanout
    outgoing = (
        jnp.zeros((received_rows, features), jnp.bfloat16).at[target].set(tokens[source_token])
    )
    outgoing = outgoing.reshape(members, capacity, features)
    gate_proj, up_proj, down_proj = (gate_weight[0], up_weight[0], down_weight[0])
    arrived = lax.all_to_all(outgoing, "ep", split_axis=0, concat_axis=0, tiled=True)
    shape_here = arrived.shape
    answers = run_expert_block(
        arrived.reshape(-1, features), gate_proj, up_proj, down_proj
    ).reshape(shape_here)
    returned = lax.all_to_all(answers, "ep", split_axis=0, concat_axis=0, tiled=True)
    selected_experts = (
        returned.reshape(-1, features)[target]
        .astype(jnp.float32)
        .reshape(tokens_here, fanout, features)
    )
    mixture = jnp.sum(selected_experts * combine[:, :, None], axis=1)
    return mixture.astype(jnp.bfloat16)


def solution(mesh):
    in_specs = (
        P(("groups", "ep"), None),
        P(("groups", "ep"), None),
        P(("groups", "ep"), None),
        P("ep", None, None),
        P("ep", None, None),
        P("ep", None, None),
    )
    out_specs = P(("groups", "ep"), None)
    return jax.shard_map(
        on_device, mesh=mesh, in_specs=in_specs, out_specs=out_specs, check_vma=False
    )
```

```python
import functools

import jax
import jax.numpy as jnp
from jax import lax
from jax.experimental import pallas as pl
from jax.experimental.pallas import tpu as pltpu
from jax.sharding import PartitionSpec as P

MESH = pl.DeviceIdType.MESH

alpha_gate = 1.702


def run_expert_block(row_block, gate_proj, up_proj, down_proj):
    gate_part = jnp.dot(row_block, gate_proj, preferred_element_type=jnp.float32)
    up_part = jnp.dot(row_block, up_proj, preferred_element_type=jnp.float32)
    hidden = ((up_part + 1.0) * gate_part * jax.nn.sigmoid(alpha_gate * gate_part)).astype(
        jnp.bfloat16
    )
    return jnp.dot(hidden, down_proj, preferred_element_type=jnp.float32).astype(jnp.bfloat16)


def line_kernel(
    tok_hbm, mix_ref, gate_hbm, up_hbm, down_hbm, out_ref,
    x_buf, w_in, gate_w, up_w, down_w, rows, part, other, quad, rx, ru, rd,
    load_sem, agz_s, agx_s, agp_s, w_s, pc_s, rsx_s, rsz_s,
    x_r, w_r, q_r, rx_r, ru_r, rd_r,
    *, members, capacity,
):
    length = members // 4
    here = tok_hbm.shape[0]
    me = lax.axis_index("ep")
    z, x, c = me // 4, (me // 2) % 2, me % 2
    pc = 1 - c

    def member(zz, xx, cc):
        return (zz * 2 + xx) * 2 + cc

    across = member(z, 1 - x, c)
    partner = member(z, x, pc)
    above = member(jnp.minimum(z + 1, length - 1), x, c)
    below = member(jnp.maximum(z - 1, 0), x, c)

    def send(src, dst, ssem, rsem, to):
        return pltpu.make_async_remote_copy(
            src_ref=src, dst_ref=dst, send_sem=ssem, recv_sem=rsem,
            device_id={"ep": to}, device_id_type=MESH,
        )

    loads = [
        pltpu.make_async_copy(tok_hbm, x_buf.at[z, x, c], load_sem.at[0]),
        pltpu.make_async_copy(gate_hbm, gate_w, load_sem.at[1]),
        pltpu.make_async_copy(up_hbm, up_w, load_sem.at[2]),
        pltpu.make_async_copy(down_hbm, down_w, load_sem.at[3]),
    ]
    for load in loads:
        load.start()

    barrier = pltpu.get_barrier_semaphore()
    for step in range(1, members):
        to = lax.rem(me + step, members)
        pl.semaphore_signal(barrier, inc=1, device_id={"ep": to}, device_id_type=MESH)
    pl.semaphore_wait(barrier, members - 1)

    def weights_copy(step):
        to = lax.rem(me + step, members)
        return send(mix_ref.at[to], w_in.at[me], w_s.at[step], w_r.at[me], to)

    def weights_arrival(step):
        origin = lax.rem(me + step, members)
        return send(mix_ref.at[origin], w_in.at[origin], w_s.at[step], w_r.at[origin], origin)

    def ag(zz, xx, ssem, to):
        slot = x_buf.at[zz, xx, c]
        return send(slot, slot, ssem, x_r.at[zz, xx, c], to)

    def to_above(zz):
        return ag(zz, x, agz_s.at[zz, 0], above)

    def to_below(zz):
        return ag(zz, x, agz_s.at[zz, 1], below)

    def to_across(zz):
        return ag(zz, x, agx_s.at[zz], across)

    def to_partner(zz, xx):
        return ag(zz, xx, agp_s.at[zz, xx], partner)

    def goes_up(zz):
        return jnp.logical_and(zz <= z, z < length - 1)

    def goes_down(zz):
        return jnp.logical_and(zz >= z, z > 0)

    def forward(zz):
        @pl.when(goes_up(zz))
        def _():
            to_above(zz).start()

        @pl.when(goes_down(zz))
        def _():
            to_below(zz).start()

        to_across(zz).start()
        to_partner(zz, x).start()

    def arrival(zz, xx, cc):
        slot = x_buf.at[zz, xx, cc]
        send(slot, slot, agx_s.at[zz], x_r.at[zz, xx, cc], partner).wait_recv()

    near = jnp.minimum(z, length - 1 - z)

    def nearest(k):
        along = near + jnp.where(k % 2 == 1, (k + 1) // 2, -(k // 2))
        low = jnp.where(k <= 2 * near, along, k)
        return jnp.where(z == near, low, length - 1 - low)

    loads[0].wait()
    forward(z)
    for step in range(1, members):
        weights_copy(step).start()
    w_in[me] = mix_ref[me]
    for step in range(1, members):
        weights_arrival(step).wait_recv()

    row_at = lax.broadcasted_iota(jnp.int32, (capacity, here), 0).astype(jnp.float32)
    before = (
        lax.broadcasted_iota(jnp.int32, (here, here), 0)
        < lax.broadcasted_iota(jnp.int32, (here, here), 1)
    ).astype(jnp.bfloat16)

    def picker(zz, xx, cc):
        weight = w_in[member(zz, xx, cc)]
        named = weight > 0.0
        flags = jnp.broadcast_to(named.astype(jnp.float32), (8, here)).astype(jnp.bfloat16)
        rank = jnp.dot(flags, before, preferred_element_type=jnp.float32)[0:1, :]
        pick = jnp.where(named, rank, -1.0) == row_at
        scale = jnp.sum(jnp.where(pick, weight, 0.0), axis=1, keepdims=True)
        return pick.astype(jnp.float32).astype(jnp.bfloat16), scale

    def compute(zz, xx):
        picks, scales = [], []
        for side, cc in enumerate((c, pc)):
            pick, scale = picker(zz, xx, cc)
            picks.append(pick)
            scales.append(scale)
            rows[side * capacity : (side + 1) * capacity, :] = jnp.dot(
                pick, x_buf[zz, xx, cc], preferred_element_type=jnp.float32
            ).astype(jnp.bfloat16)
        block = rows[...]
        gate = jnp.dot(block, gate_w[...], preferred_element_type=jnp.float32)
        up = jnp.dot(block, up_w[...], preferred_element_type=jnp.float32)
        hidden = ((up + 1.0) * gate * jax.nn.sigmoid(alpha_gate * gate)).astype(jnp.bfloat16)
        answer = jnp.dot(hidden, down_w[...], preferred_element_type=jnp.float32)
        for side, dst in enumerate((part, other)):
            scaled = (
                answer[side * capacity : (side + 1) * capacity, :]
                .astype(jnp.bfloat16).astype(jnp.float32) * scales[side]
            ).astype(jnp.bfloat16)
            dst[zz, xx] = lax.dot_general(
                picks[side], scaled, (((0,), (0,)), ((), ())),
                preferred_element_type=jnp.float32,
            ).astype(jnp.bfloat16)

    def answer_copy(zz, xx):
        return send(other.at[zz, xx], quad.at[zz, xx], pc_s.at[zz, xx], q_r.at[zz, xx], partner)

    def across_copy(zz):
        return send(part.at[zz, 1 - x], rx.at[zz], rsx_s.at[zz], rx_r.at[zz], across)

    def join_partner(zz, xx):
        answer_copy(zz, xx).wait_recv()
        part[zz, xx] = (
            part[zz, xx].astype(jnp.float32) + quad[zz, xx].astype(jnp.float32)
        ).astype(jnp.bfloat16)

    def up_copy(zz, xx):
        return send(part.at[zz, xx], ru.at[zz, xx], rsz_s.at[zz, xx], ru_r.at[zz, xx], above)

    def down_copy(zz, xx):
        return send(part.at[zz, xx], rd.at[zz, xx], rsz_s.at[zz, xx], rd_r.at[zz, xx], below)

    def add_in(zz, xx, addend):
        part[zz, xx] = (
            part[zz, xx].astype(jnp.float32) + addend.astype(jnp.float32)
        ).astype(jnp.bfloat16)

    def take_across(zz):
        across_copy(zz).wait_recv()
        add_in(zz, x, rx[zz])

    def column(j):
        return jnp.where(c == 1, x, (x + 1 + j) % 2)

    def chain(zz):
        @pl.when(c == 1)
        def _():
            take_across(zz)

        def one(j, carry):
            xx = column(j)

            @pl.when(jnp.logical_and(zz >= z, z > 0))
            def _():
                up_copy(zz, xx).wait_recv()
                add_in(zz, xx, ru[zz, xx])

            @pl.when(jnp.logical_and(zz <= z, z < length - 1))
            def _():
                down_copy(zz, xx).wait_recv()
                add_in(zz, xx, rd[zz, xx])

            @pl.when(zz > z)
            def _():
                up_copy(zz, xx).start()

            @pl.when(zz < z)
            def _():
                down_copy(zz, xx).start()

            @pl.when(jnp.logical_and(zz == z, xx != x))
            def _():
                across_copy(zz).start()

            return carry

        lax.fori_loop(0, 2 - c, one, 0)

    def starts(k):
        return jnp.logical_and(near == 0, k >= 1)

    for load in loads[1:]:
        load.wait()

    def step_of(i, carry):
        k, o = i // 2, i % 2
        zz, xx = nearest(k), (x + o) % 2

        @pl.when(o == 1)
        def _():
            @pl.when(k + 1 < length)
            def _():
                following = nearest(k + 1)
                arrival(following, x, c)
                forward(following)

            arrival(zz, 1 - x, c)
            to_partner(zz, 1 - x).start()

        arrival(zz, xx, pc)
        compute(zz, xx)
        answer_copy(zz, xx).start()

        @pl.when(i > 0)
        def _():
            last = nearest((i - 1) // 2)
            last_x = (x + (i - 1) % 2) % 2
            join_partner(last, last_x)

            @pl.when(o == 0)
            def _():
                @pl.when(c == 1)
                def _():
                    across_copy(last).start()

                @pl.when(jnp.logical_and(c == 0, starts(k - 1)))
                def _():
                    chain(last)

        @pl.when(jnp.logical_and(jnp.logical_and(o == 1, c == 1), starts(k - 1)))
        def _():
            chain(nearest(k - 1))

        return carry

    lax.fori_loop(0, 2 * length, step_of, 0)
    final = nearest(length - 1)
    join_partner(final, 1 - x)

    @pl.when(c == 1)
    def _():
        across_copy(final).start()

    def rest(i, carry):
        k = length - 1 - i

        @pl.when(jnp.logical_not(starts(k)) | (k == length - 1))
        def _():
            chain(nearest(k))

        return carry

    lax.fori_loop(0, length, rest, 0)

    @pl.when(c == 0)
    def _():
        take_across(z)

    out_ref[...] = part[z, x]

    for step in range(1, members):
        weights_copy(step).wait_send()

    def drain(zz, carry):
        @pl.when(goes_up(zz))
        def _():
            to_above(zz).wait_send()

        @pl.when(goes_down(zz))
        def _():
            to_below(zz).wait_send()

        to_across(zz).wait_send()

        @pl.when(jnp.logical_or(c == 1, zz == z))
        def _():
            across_copy(zz).wait_send()

        @pl.when(zz != z)
        def _():
            def one(j, inner):
                up_copy(zz, column(j)).wait_send()
                return inner

            lax.fori_loop(0, 2 - c, one, 0)

        for xx in range(2):
            to_partner(zz, xx).wait_send()
            answer_copy(zz, xx).wait_send()
        return carry

    lax.fori_loop(0, length, drain, 0)


def gathered_plan(tokens, expert_ids, combine, gate_proj, up_proj, down_proj, capacity):
    members = lax.axis_size("ep")
    here, features = tokens.shape
    ff = gate_proj.shape[1]
    length = members // 4
    experts = jnp.arange(members, dtype=jnp.int32)[:, None, None]
    ids, shares = expert_ids.T[None], combine.T[None]
    mix = jnp.sum(jnp.where(ids == experts, shares, 0.0), axis=1, keepdims=True)
    block = (here, features)
    dma = pltpu.SemaphoreType.DMA
    vmem = lambda *shape: pltpu.VMEM(shape, jnp.bfloat16)
    anywhere = pl.BlockSpec(memory_space=pl.ANY)
    inside = pl.BlockSpec(memory_space=pltpu.VMEM)
    return pl.pallas_call(
        functools.partial(line_kernel, members=members, capacity=capacity),
        out_shape=jax.ShapeDtypeStruct(block, jnp.bfloat16),
        in_specs=[anywhere, inside, anywhere, anywhere, anywhere],
        out_specs=inside,
        scratch_shapes=[
            vmem(length, 2, 2, *block),
            pltpu.VMEM((members, 1, here), jnp.float32),
            vmem(features, ff), vmem(features, ff), vmem(ff, features),
            vmem(2 * capacity, features),
            vmem(length, 2, *block), vmem(length, 2, *block), vmem(length, 2, *block),
            vmem(length, *block), vmem(length, 2, *block), vmem(length, 2, *block),
            dma((4,)), dma((length, 2)), dma((length,)), dma((length, 2)), dma((members,)),
            dma((length, 2)), dma((length,)), dma((length, 2)),
            dma((length, 2, 2)), dma((members,)), dma((length, 2)),
            dma((length,)), dma((length, 2)), dma((length, 2)),
        ],
        compiler_params=pltpu.CompilerParams(
            collective_id=0, has_side_effects=True, vmem_limit_bytes=60 * 1024 * 1024
        ),
    )(tokens, mix, gate_proj, up_proj, down_proj)


def on_device(tokens, expert_ids, combine, gate_weight, up_weight, down_weight):
    members = lax.axis_size("ep")
    tokens_here, fanout = expert_ids.shape
    features = tokens.shape[1]
    capacity = 2 * tokens_here * fanout // members
    received_rows = members * capacity
    if members % 4 == 0 and 2 * capacity >= tokens_here:
        return gathered_plan(
            tokens, expert_ids, combine, gate_weight[0], up_weight[0], down_weight[0], capacity
        )
    flat_ids = expert_ids.reshape(-1)
    onehot = (flat_ids[:, None] == jnp.arange(members, dtype=jnp.int32)[None, :]).astype(jnp.int32)
    running = jnp.cumsum(onehot, axis=0) - onehot
    slot_rank = jnp.sum(running * onehot, axis=1)
    target = flat_ids * capacity + slot_rank
    source_token = jnp.arange(tokens_here * fanout, dtype=jnp.int32) // fanout
    outgoing = (
        jnp.zeros((received_rows, features), jnp.bfloat16).at[target].set(tokens[source_token])
    )
    outgoing = outgoing.reshape(members, capacity, features)
    gate_proj, up_proj, down_proj = (gate_weight[0], up_weight[0], down_weight[0])
    arrived = lax.all_to_all(outgoing, "ep", split_axis=0, concat_axis=0, tiled=True)
    shape_here = arrived.shape
    answers = run_expert_block(
        arrived.reshape(-1, features), gate_proj, up_proj, down_proj
    ).reshape(shape_here)
    returned = lax.all_to_all(answers, "ep", split_axis=0, concat_axis=0, tiled=True)
    selected_experts = (
        returned.reshape(-1, features)[target]
        .astype(jnp.float32)
        .reshape(tokens_here, fanout, features)
    )
    mixture = jnp.sum(selected_experts * combine[:, :, None], axis=1)
    return mixture.astype(jnp.bfloat16)


def solution(mesh):
    in_specs = (
        P(("groups", "ep"), None),
        P(("groups", "ep"), None),
        P(("groups", "ep"), None),
        P("ep", None, None),
        P("ep", None, None),
        P("ep", None, None),
    )
    out_specs = P(("groups", "ep"), None)
    return jax.shard_map(
        on_device, mesh=mesh, in_specs=in_specs, out_specs=out_specs, check_vma=False
    )
```

```python
import functools

import jax
import jax.numpy as jnp
from jax import lax
from jax.experimental import pallas as pl
from jax.experimental.pallas import tpu as pltpu
from jax.sharding import PartitionSpec as P

MESH = pl.DeviceIdType.MESH

alpha_gate = 1.702


def run_expert_block(row_block, gate_proj, up_proj, down_proj):
    gate_part = jnp.dot(row_block, gate_proj, preferred_element_type=jnp.float32)
    up_part = jnp.dot(row_block, up_proj, preferred_element_type=jnp.float32)
    hidden = ((up_part + 1.0) * gate_part * jax.nn.sigmoid(alpha_gate * gate_part)).astype(
        jnp.bfloat16
    )
    return jnp.dot(hidden, down_proj, preferred_element_type=jnp.float32).astype(jnp.bfloat16)


def line_kernel(
    tok_hbm, mix_ref, gate_hbm, up_hbm, down_hbm, out_ref,
    x_buf, w_in, gate_w, up_w, down_w, rows, part, other, quad, rx, ru, rd,
    load_sem, agz_s, agx_s, agp_s, w_s, pc_s, rsx_s, rsz_s,
    x_r, xp_r, w_r, q_r, rx_r, ru_r, rd_r,
    *, members, capacity, pieces,
):
    length = members // 4
    here = tok_hbm.shape[0]
    me = lax.axis_index("ep")
    z, x, c = me // 4, (me // 2) % 2, me % 2
    pc = 1 - c

    def member(zz, xx, cc):
        return (zz * 2 + xx) * 2 + cc

    across = member(z, 1 - x, c)
    partner = member(z, x, pc)
    above = member(jnp.minimum(z + 1, length - 1), x, c)
    below = member(jnp.maximum(z - 1, 0), x, c)

    def send(src, dst, ssem, rsem, to):
        return pltpu.make_async_remote_copy(
            src_ref=src, dst_ref=dst, send_sem=ssem, recv_sem=rsem,
            device_id={"ep": to}, device_id_type=MESH,
        )

    loads = [
        pltpu.make_async_copy(tok_hbm, x_buf.at[z, x, c], load_sem.at[0]),
        pltpu.make_async_copy(gate_hbm, gate_w, load_sem.at[1]),
        pltpu.make_async_copy(up_hbm, up_w, load_sem.at[2]),
        pltpu.make_async_copy(down_hbm, down_w, load_sem.at[3]),
    ]
    for load in loads:
        load.start()

    barrier = pltpu.get_barrier_semaphore()
    for step in range(1, members):
        to = lax.rem(me + step, members)
        pl.semaphore_signal(barrier, inc=1, device_id={"ep": to}, device_id_type=MESH)
    pl.semaphore_wait(barrier, members - 1)

    def weights_copy(step):
        to = lax.rem(me + step, members)
        return send(mix_ref.at[to], w_in.at[me], w_s.at[step], w_r.at[me], to)

    def weights_arrival(step):
        origin = lax.rem(me + step, members)
        return send(mix_ref.at[origin], w_in.at[origin], w_s.at[step], w_r.at[origin], origin)

    size = here // pieces

    def cut(piece):
        return pl.ds(pl.multiple_of(piece * size, size), size)

    def ag(zz, piece, ssem, to):
        slot = x_buf.at[zz, x, c, cut(piece)]
        return send(slot, slot, ssem, x_r.at[zz, x, piece], to)

    def to_above(zz, piece):
        return ag(zz, piece, agz_s.at[zz, 0, piece], above)

    def to_below(zz, piece):
        return ag(zz, piece, agz_s.at[zz, 1, piece], below)

    def to_across(zz, piece):
        return ag(zz, piece, agx_s.at[zz, piece], across)

    def to_partner(zz, xx):
        slot = x_buf.at[zz, xx, c]
        return send(slot, slot, agp_s.at[zz, xx], xp_r.at[zz, xx], partner)

    def goes_up(zz):
        return jnp.logical_and(zz <= z, z < length - 1)

    def goes_down(zz):
        return jnp.logical_and(zz >= z, z > 0)

    def each_piece(act):
        def one(piece, carry):
            act(piece)
            return carry

        lax.fori_loop(0, pieces, one, 0)

    def forward(zz, arriving):
        def one(piece):
            if arriving:
                arrival(zz, x, piece)

            @pl.when(goes_up(zz))
            def _():
                to_above(zz, piece).start()

            @pl.when(goes_down(zz))
            def _():
                to_below(zz, piece).start()

            to_across(zz, piece).start()

        each_piece(one)
        to_partner(zz, x).start()

    def arrival(zz, xx, piece):
        slot = x_buf.at[zz, xx, c, cut(piece)]
        send(slot, slot, agx_s.at[zz, piece], x_r.at[zz, xx, piece], partner).wait_recv()

    def partner_arrival(zz, xx):
        slot = x_buf.at[zz, xx, pc]
        send(slot, slot, agp_s.at[zz, xx], xp_r.at[zz, xx], partner).wait_recv()

    near = jnp.minimum(z, length - 1 - z)

    def nearest(k):
        along = near + jnp.where(k % 2 == 1, (k + 1) // 2, -(k // 2))
        low = jnp.where(k <= 2 * near, along, k)
        return jnp.where(z == near, low, length - 1 - low)

    loads[0].wait()
    forward(z, False)
    for step in range(1, members):
        weights_copy(step).start()
    w_in[me] = mix_ref[me]
    for step in range(1, members):
        weights_arrival(step).wait_recv()

    row_at = lax.broadcasted_iota(jnp.int32, (capacity, here), 0).astype(jnp.float32)
    before = (
        lax.broadcasted_iota(jnp.int32, (here, here), 0)
        < lax.broadcasted_iota(jnp.int32, (here, here), 1)
    ).astype(jnp.bfloat16)

    def picker(zz, xx, cc):
        weight = w_in[member(zz, xx, cc)]
        named = weight > 0.0
        flags = jnp.broadcast_to(named.astype(jnp.float32), (8, here)).astype(jnp.bfloat16)
        rank = jnp.dot(flags, before, preferred_element_type=jnp.float32)[0:1, :]
        pick = jnp.where(named, rank, -1.0) == row_at
        scale = jnp.sum(jnp.where(pick, weight, 0.0), axis=1, keepdims=True)
        return pick.astype(jnp.float32).astype(jnp.bfloat16), scale

    def compute(zz, xx):
        picks, scales = [], []
        for side, cc in enumerate((c, pc)):
            pick, scale = picker(zz, xx, cc)
            picks.append(pick)
            scales.append(scale)
            rows[side * capacity : (side + 1) * capacity, :] = jnp.dot(
                pick, x_buf[zz, xx, cc], preferred_element_type=jnp.float32
            ).astype(jnp.bfloat16)
        block = rows[...]
        gate = jnp.dot(block, gate_w[...], preferred_element_type=jnp.float32)
        up = jnp.dot(block, up_w[...], preferred_element_type=jnp.float32)
        hidden = ((up + 1.0) * gate * jax.nn.sigmoid(alpha_gate * gate)).astype(jnp.bfloat16)
        answer = jnp.dot(hidden, down_w[...], preferred_element_type=jnp.float32)
        for side, dst in enumerate((part, other)):
            scaled = (
                answer[side * capacity : (side + 1) * capacity, :]
                .astype(jnp.bfloat16).astype(jnp.float32) * scales[side]
            ).astype(jnp.bfloat16)
            dst[zz, xx] = lax.dot_general(
                picks[side], scaled, (((0,), (0,)), ((), ())),
                preferred_element_type=jnp.float32,
            ).astype(jnp.bfloat16)

    def answer_copy(zz, xx):
        return send(other.at[zz, xx], quad.at[zz, xx], pc_s.at[zz, xx], q_r.at[zz, xx], partner)

    def across_copy(zz, piece):
        return send(
            part.at[zz, 1 - x, cut(piece)], rx.at[zz, cut(piece)],
            rsx_s.at[zz, piece], rx_r.at[zz, piece], across,
        )

    def all_across(zz):
        each_piece(lambda piece: across_copy(zz, piece).start())

    def join_partner(zz, xx):
        answer_copy(zz, xx).wait_recv()
        part[zz, xx] = (
            part[zz, xx].astype(jnp.float32) + quad[zz, xx].astype(jnp.float32)
        ).astype(jnp.bfloat16)

    def up_copy(zz, xx, piece):
        return send(
            part.at[zz, xx, cut(piece)], ru.at[zz, xx, cut(piece)],
            rsz_s.at[zz, xx, piece], ru_r.at[zz, xx, piece], above,
        )

    def down_copy(zz, xx, piece):
        return send(
            part.at[zz, xx, cut(piece)], rd.at[zz, xx, cut(piece)],
            rsz_s.at[zz, xx, piece], rd_r.at[zz, xx, piece], below,
        )

    def add_in(zz, xx, piece, addend):
        part[zz, xx, cut(piece)] = (
            part[zz, xx, cut(piece)].astype(jnp.float32) + addend.astype(jnp.float32)
        ).astype(jnp.bfloat16)

    def take_across(zz, piece):
        across_copy(zz, piece).wait_recv()
        add_in(zz, x, piece, rx[zz, cut(piece)])

    def column(j):
        return jnp.where(c == 1, x, (x + 1 + j) % 2)

    def chain(zz):
        def one(step, carry):
            xx, piece = column(step // pieces), step % pieces

            @pl.when(c == 1)
            def _():
                take_across(zz, piece)

            @pl.when(jnp.logical_and(zz >= z, z > 0))
            def _():
                up_copy(zz, xx, piece).wait_recv()
                add_in(zz, xx, piece, ru[zz, xx, cut(piece)])

            @pl.when(jnp.logical_and(zz <= z, z < length - 1))
            def _():
                down_copy(zz, xx, piece).wait_recv()
                add_in(zz, xx, piece, rd[zz, xx, cut(piece)])

            @pl.when(zz > z)
            def _():
                up_copy(zz, xx, piece).start()

            @pl.when(zz < z)
            def _():
                down_copy(zz, xx, piece).start()

            @pl.when(jnp.logical_and(zz == z, xx != x))
            def _():
                across_copy(zz, piece).start()

            return carry

        lax.fori_loop(0, (2 - c) * pieces, one, 0)

    def starts(k):
        return jnp.logical_and(near == 0, k >= 1)

    for load in loads[1:]:
        load.wait()

    def step_of(i, carry):
        k, o = i // 2, i % 2
        zz, xx = nearest(k), (x + o) % 2

        @pl.when(o == 1)
        def _():
            @pl.when(k + 1 < length)
            def _():
                following = nearest(k + 1)
                forward(following, True)

            each_piece(lambda piece: arrival(zz, 1 - x, piece))
            to_partner(zz, 1 - x).start()

        partner_arrival(zz, xx)
        compute(zz, xx)
        answer_copy(zz, xx).start()

        @pl.when(i > 0)
        def _():
            last = nearest((i - 1) // 2)
            last_x = (x + (i - 1) % 2) % 2
            join_partner(last, last_x)

            @pl.when(o == 0)
            def _():
                @pl.when(c == 1)
                def _():
                    all_across(last)

                @pl.when(jnp.logical_and(c == 0, starts(k - 1)))
                def _():
                    chain(last)

        @pl.when(jnp.logical_and(jnp.logical_and(o == 1, c == 1), starts(k - 1)))
        def _():
            chain(nearest(k - 1))

        @pl.when(jnp.logical_and(near == 1, i == 2 * length - 1))
        def _():
            chain(nearest(1))

        return carry

    lax.fori_loop(0, 2 * length, step_of, 0)
    final = nearest(length - 1)
    join_partner(final, 1 - x)

    @pl.when(c == 1)
    def _():
        all_across(final)

    def rest(i, carry):
        k = length - 1 - i

        early = jnp.logical_or(
            jnp.logical_and(starts(k), k < length - 1), jnp.logical_and(near == 1, k == 1)
        )

        @pl.when(jnp.logical_not(early))
        def _():
            chain(nearest(k))

        return carry

    lax.fori_loop(0, length, rest, 0)

    @pl.when(c == 0)
    def _():
        each_piece(lambda piece: take_across(z, piece))

    out_ref[...] = part[z, x]

    for step in range(1, members):
        weights_copy(step).wait_send()

    def drain(zz, carry):
        def one(piece):
            @pl.when(goes_up(zz))
            def _():
                to_above(zz, piece).wait_send()

            @pl.when(goes_down(zz))
            def _():
                to_below(zz, piece).wait_send()

            to_across(zz, piece).wait_send()

            @pl.when(jnp.logical_or(c == 1, zz == z))
            def _():
                across_copy(zz, piece).wait_send()

            @pl.when(zz != z)
            def _():
                up_copy(zz, x, piece).wait_send()

            @pl.when(jnp.logical_and(zz != z, c == 0))
            def _():
                up_copy(zz, 1 - x, piece).wait_send()

        each_piece(one)
        for xx in range(2):
            to_partner(zz, xx).wait_send()
            answer_copy(zz, xx).wait_send()
        return carry

    lax.fori_loop(0, length, drain, 0)


def gathered_plan(tokens, expert_ids, combine, gate_proj, up_proj, down_proj, capacity):
    members = lax.axis_size("ep")
    here, features = tokens.shape
    ff = gate_proj.shape[1]
    length = members // 4
    pieces = 4 if here % 64 == 0 else 1
    experts = jnp.arange(members, dtype=jnp.int32)[:, None, None]
    ids, shares = expert_ids.T[None], combine.T[None]
    mix = jnp.sum(jnp.where(ids == experts, shares, 0.0), axis=1, keepdims=True)
    block = (here, features)
    dma = pltpu.SemaphoreType.DMA
    vmem = lambda *shape: pltpu.VMEM(shape, jnp.bfloat16)
    anywhere = pl.BlockSpec(memory_space=pl.ANY)
    inside = pl.BlockSpec(memory_space=pltpu.VMEM)
    return pl.pallas_call(
        functools.partial(line_kernel, members=members, capacity=capacity, pieces=pieces),
        out_shape=jax.ShapeDtypeStruct(block, jnp.bfloat16),
        in_specs=[anywhere, inside, anywhere, anywhere, anywhere],
        out_specs=inside,
        scratch_shapes=[
            vmem(length, 2, 2, *block),
            pltpu.VMEM((members, 1, here), jnp.float32),
            vmem(features, ff), vmem(features, ff), vmem(ff, features),
            vmem(2 * capacity, features),
            vmem(length, 2, *block), vmem(length, 2, *block), vmem(length, 2, *block),
            vmem(length, *block), vmem(length, 2, *block), vmem(length, 2, *block),
            dma((4,)), dma((length, 2, pieces)), dma((length, pieces)), dma((length, 2)),
            dma((members,)),
            dma((length, 2)), dma((length, pieces)), dma((length, 2, pieces)),
            dma((length, 2, pieces)), dma((length, 2)), dma((members,)), dma((length, 2)),
            dma((length, pieces)), dma((length, 2, pieces)), dma((length, 2, pieces)),
        ],
        compiler_params=pltpu.CompilerParams(
            collective_id=0, has_side_effects=True, vmem_limit_bytes=60 * 1024 * 1024
        ),
    )(tokens, mix, gate_proj, up_proj, down_proj)


def on_device(tokens, expert_ids, combine, gate_weight, up_weight, down_weight):
    members = lax.axis_size("ep")
    tokens_here, fanout = expert_ids.shape
    features = tokens.shape[1]
    capacity = 2 * tokens_here * fanout // members
    received_rows = members * capacity
    if members % 4 == 0 and 2 * capacity >= tokens_here:
        return gathered_plan(
            tokens, expert_ids, combine, gate_weight[0], up_weight[0], down_weight[0], capacity
        )
    flat_ids = expert_ids.reshape(-1)
    onehot = (flat_ids[:, None] == jnp.arange(members, dtype=jnp.int32)[None, :]).astype(jnp.int32)
    running = jnp.cumsum(onehot, axis=0) - onehot
    slot_rank = jnp.sum(running * onehot, axis=1)
    target = flat_ids * capacity + slot_rank
    source_token = jnp.arange(tokens_here * fanout, dtype=jnp.int32) // fanout
    outgoing = (
        jnp.zeros((received_rows, features), jnp.bfloat16).at[target].set(tokens[source_token])
    )
    outgoing = outgoing.reshape(members, capacity, features)
    gate_proj, up_proj, down_proj = (gate_weight[0], up_weight[0], down_weight[0])
    arrived = lax.all_to_all(outgoing, "ep", split_axis=0, concat_axis=0, tiled=True)
    shape_here = arrived.shape
    answers = run_expert_block(
        arrived.reshape(-1, features), gate_proj, up_proj, down_proj
    ).reshape(shape_here)
    returned = lax.all_to_all(answers, "ep", split_axis=0, concat_axis=0, tiled=True)
    selected_experts = (
        returned.reshape(-1, features)[target]
        .astype(jnp.float32)
        .reshape(tokens_here, fanout, features)
    )
    mixture = jnp.sum(selected_experts * combine[:, :, None], axis=1)
    return mixture.astype(jnp.bfloat16)


def solution(mesh):
    in_specs = (
        P(("groups", "ep"), None),
        P(("groups", "ep"), None),
        P(("groups", "ep"), None),
        P("ep", None, None),
        P("ep", None, None),
        P("ep", None, None),
    )
    out_specs = P(("groups", "ep"), None)
    return jax.shard_map(
        on_device, mesh=mesh, in_specs=in_specs, out_specs=out_specs, check_vma=False
    )
```
